32 devices in a mesh: job: 4 (over y, x), zero: 2 (over core), cols: 4 (over z).
Axes of the slice: x: 2, y: 2, z: 4, core: 2. Of those that a mesh axis runs over, the one named last changes fastest.
Arguments:
- weight_query: bfloat16 [12288, 3072], P(('job', 'zero'), 'cols'), parts along dimension 0, may hold values from -0.109375 to 0.109375
- low_query: bfloat16 [12288, 32], P(('job', 'zero')), parts along dimension 0, may hold values from -0.109375 to 0.109375
- high_query: bfloat16 [128, 3072], P('job', 'cols'), parts along dimension 0, may hold values from -1 to 1
- weight_key: bfloat16 [12288, 1024], P(('job', 'zero'), 'cols'), parts along dimension 0, may hold values from -0.109375 to 0.109375
- low_key: bfloat16 [12288, 32], P(('job', 'zero')), parts along dimension 0, may hold values from -0.109375 to 0.109375
- high_key: bfloat16 [128, 1024], P('job', 'cols'), parts along dimension 0, may hold values from -1 to 1
- weight_value: bfloat16 [12288, 1024], P(('job', 'zero'), 'cols'), parts along dimension 0, may hold values from -0.109375 to 0.109375
- low_value: bfloat16 [12288, 32], P(('job', 'zero')), parts along dimension 0, may hold values from -0.109375 to 0.109375
- high_value: bfloat16 [128, 1024], P('job', 'cols'), parts along dimension 0, may hold values from -1 to 1
- weight_mixed: bfloat16 [12288, 3072], P(('job', 'cols'), 'zero'), parts along dimension 0, may hold values from -0.109375 to 0.109375
- low_mixed: bfloat16 [12288, 32], P(('job', 'cols')), parts along dimension 0, may hold values from -0.109375 to 0.109375
- high_mixed: bfloat16 [128, 3072], P('job', 'zero'), parts along dimension 0, may hold values from -1 to 1
- norm_train: float32 [12288], P(('job', 'zero', 'cols')), parts along dimension 0, may hold values from 0.25 to 1.75
- norm_step: float32 [12288], P(('job', 'zero', 'cols')), parts along dimension 0, may hold values from -0.3 to 0.3
Outputs:
- serving_query: bfloat16 [12288, 3072], P('job', 'cols'), parts along dimension 0
- serving_key: bfloat16 [12288, 1024], P('job', 'cols'), parts along dimension 0
- serving_value: bfloat16 [12288, 1024], P('job', 'cols'), parts along dimension 0
- serving_mixed: bfloat16 [12288, 3072], P(('job', 'cols')), parts along dimension 0
- serve_norm: bfloat16 [12288], P('job'), parts along dimension 0
The draws below stay inside these ranges and needn't reach their ends.
There are 4 independent parts, one for each index of `job`. The reference program is written for one: setup_inputs(seed, part) draws one part's arguments, and reference() takes and returns one part's arrays. A program takes and returns all parts, laid end to end along the dimension named above; each array names one. Nothing has to cross between parts.
All inputs are finite; a program needn't handle non-finite values.
Results may differ from the reference program's by a relative error of at most 0.001.
Values may be sent and summed in bfloat16 or wider, within the bound.
A program may use at most 128 MiB of HBM per device.

```python
import jax
import jax.numpy as jnp

D_MODEL = 3072
Q_DIM = 3072
KV_DIM = 1024
RANK = 32


def shard_levels(own_key, extent, split, smallest, high):
    def one(axis_at, shards_of):
        draws = jax.random.uniform(jax.random.fold_in(jax.random.fold_in(own_key, 6), axis_at), (shards_of,), jnp.float32, smallest / len(split), high / len(split))
        return jnp.repeat(jnp.exp(draws), extent[axis_at] // shards_of).reshape((-1,) + (1,) * (len(extent) - axis_at - 1))

    loudness = one(*split[0])
    for cut in split[1:]:
        loudness = loudness * one(*cut)
    return loudness


def bell_draw(stream_key, dims, spread, most, cuts=(), dtype=jnp.bfloat16):
    gain = shard_levels(stream_key, dims, cuts, -0.22, 0.18) if cuts else 1.0
    drawn = jax.random.normal(stream_key, dims, jnp.float32) * spread * gain
    return jnp.minimum(jnp.maximum(drawn, -most), most).astype(dtype)


def setup_inputs(seed: int = 0, part: int = 0) -> dict:
    arg_keys = jax.random.split(jax.random.key(seed), 15)
    own_keys = jax.random.split(jax.random.fold_in(arg_keys[14], part), 15)
    return {
        "weight_query": bell_draw(own_keys[0], (D_MODEL, Q_DIM), D_MODEL ** -0.5, 0.109375, ((0, 2), (1, 4))),
        "low_query": bell_draw(own_keys[1], (D_MODEL, RANK), D_MODEL ** -0.5, 0.109375, ((0, 2),)),
        "high_query": bell_draw(own_keys[2], (RANK, Q_DIM), RANK ** -0.5, 1.0, ((1, 4),)),
        "weight_key": bell_draw(own_keys[3], (D_MODEL, KV_DIM), D_MODEL ** -0.5, 0.109375, ((0, 2), (1, 4))),
        "low_key": bell_draw(own_keys[4], (D_MODEL, RANK), D_MODEL ** -0.5, 0.109375, ((0, 2),)),
        "high_key": bell_draw(own_keys[5], (RANK, KV_DIM), RANK ** -0.5, 1.0, ((1, 4),)),
        "weight_value": bell_draw(own_keys[6], (D_MODEL, KV_DIM), D_MODEL ** -0.5, 0.109375, ((0, 2), (1, 4))),
        "low_value": bell_draw(own_keys[7], (D_MODEL, RANK), D_MODEL ** -0.5, 0.109375, ((0, 2),)),
        "high_value": bell_draw(own_keys[8], (RANK, KV_DIM), RANK ** -0.5, 1.0, ((1, 4),)),
        "weight_mixed": bell_draw(own_keys[9], (Q_DIM, D_MODEL), Q_DIM ** -0.5, 0.109375, ((0, 4), (1, 2))),
        "low_mixed": bell_draw(own_keys[10], (Q_DIM, RANK), Q_DIM ** -0.5, 0.109375, ((0, 4),)),
        "high_mixed": bell_draw(own_keys[11], (RANK, D_MODEL), RANK ** -0.5, 1.0, ((1, 2),)),
        "norm_train": jnp.clip(1.0 + 0.15 * jax.random.normal(own_keys[12], (D_MODEL,), jnp.float32), 0.25, 1.75),
        "norm_step": jnp.clip(jax.random.uniform(own_keys[13], (D_MODEL,), jnp.float32, -0.3, 0.3) * shard_levels(own_keys[13], (D_MODEL,), ((0, 8),), -0.4, 0.0), -0.3, 0.3),
    }


mix_rate = 2.0


def reference(weight_query, low_query, high_query, weight_key, low_key, high_key, weight_value, low_value, high_value, weight_mixed, low_mixed, high_mixed, norm_train, norm_step):
    whole_query = weight_query.astype(jnp.float32) + mix_rate * jnp.dot(low_query, high_query, preferred_element_type=jnp.float32)
    whole_key = weight_key.astype(jnp.float32) + mix_rate * jnp.dot(low_key, high_key, preferred_element_type=jnp.float32)
    whole_value = weight_value.astype(jnp.float32) + mix_rate * jnp.dot(low_value, high_value, preferred_element_type=jnp.float32)
    whole_mixed = weight_mixed.astype(jnp.float32) + mix_rate * jnp.dot(low_mixed, high_mixed, preferred_element_type=jnp.float32)
    serving_query = whole_query.astype(jnp.bfloat16)
    serving_key = whole_key.astype(jnp.bfloat16)
    serving_value = whole_value.astype(jnp.bfloat16)
    serving_mixed = whole_mixed.astype(jnp.bfloat16)
    serve_norm = (norm_train + norm_step).astype(jnp.bfloat16)
    return serving_query, serving_key, serving_value, serving_mixed, serve_norm
```

```python
import functools

import jax
import jax.numpy as jnp
from jax import lax
from jax.experimental import pallas as pl
from jax.experimental.pallas import tpu as pltpu
from jax.sharding import PartitionSpec as P


mix_rate = 2.0
lanes = 128
piece_bytes = 800 * 1024


tile_rows, tile_columns = 256, 256
own_order = (1, 2, 3, 0)
send_last, ahead, read_bytes = 2, 3, 2400 * 1024
write_bytes = 400 * 1024
gain_rows, rank = 16, 32


def merge(done, shift, weight, low_t, high, at, tall):
    columns = weight.shape[1]
    wide = tile_columns if columns % tile_columns == 0 else columns
    deep = tile_rows if tall % tile_rows == 0 else tall
    for top in range(at, at + tall, deep):
        low = low_t[:, pl.ds(top, deep)] * jnp.bfloat16(mix_rate)
        for left in range(0, columns, wide):
            where = (pl.ds(top, deep), pl.ds(left, wide))
            update = lax.dot_general(
                low, high[:, pl.ds(left, wide)], (((0,), (0,)), ((), ())), preferred_element_type=jnp.float32
            )
            done[pl.ds(top, deep), pl.ds(shift + left, wide)] = (weight[where].astype(jnp.float32) + update).astype(jnp.bfloat16)


def pieces_of(shape, limit=piece_bytes):
    rows, columns = shape
    best = lanes
    for tall in range(lanes, rows + 1, lanes):
        if rows % tall == 0 and 2 * tall * columns <= limit:
            best = tall
    return [(at, best) for at in range(0, rows, best)]


def place(whole, slot, by_rows, shape, at, tall):
    rows, columns = shape
    if by_rows:
        return whole.at[pl.ds(slot * rows + at, tall), :]
    return whole.at[pl.ds(at, tall), pl.ds(pl.multiple_of(slot * columns, lanes), columns)]


def own_kernel(cols, *refs):
    (total, far_total), weights, factors = refs[:2], refs[2:6], refs[6:14]
    q_out, mix_out, m_out, low_m, high_q = refs[14:19]
    held, lows, highs = refs[19:23], (*refs[23:26], low_m), (high_q, *refs[26:29])
    mine, got, gains = refs[29:32]
    read_sem, factor_sem, pack_sem, send_sem, recv_sem = refs[32:]
    my_zero, my_col = lax.axis_index("zero"), lax.axis_index("cols")
    leads = my_zero == 1
    barrier = pltpu.get_barrier_semaphore()
    others = [{"cols": lax.rem(my_col + n, cols)} for n in range(1, cols)]

    @pl.when(leads)
    def _():
        for other in others:
            pl.semaphore_signal(barrier, inc=1, device_id=other, device_id_type=pl.DeviceIdType.MESH)

    tall = total.shape[0]
    room = mine.shape[0] // 2
    mine[pl.ds(my_zero * room, tall), :] = total[...]
    mine[pl.ds((1 - my_zero) * room, tall), :] = far_total[...]
    rows, wide = weights[1].shape
    targets = ((q_out, 0), (mix_out, 0), (mix_out, wide), (m_out, 0))
    work = [(n, at, tall) for n in own_order for at, tall in pieces_of(weights[n].shape, read_bytes)]
    reads = []
    for i, (n, at, piece) in enumerate(work):
        part = pl.ds(at, piece)
        reads.append(pltpu.make_async_copy(weights[n].at[part, :], held[n].at[part, :], read_sem.at[i]))
    loads = []
    for i, (source, target) in enumerate(zip(factors, (*lows, *highs))):
        loads.append(pltpu.make_async_copy(source, target, factor_sem.at[i]))
    below = rows + gain_rows
    packs = []
    for i in range(rows // (2 * wide)):
        target = mix_out.at[pl.ds(below + i * rank, rank), :]
        packs.append(pltpu.make_async_copy(factors[0].at[:, pl.ds(2 * i * wide, 2 * wide)], target, pack_sem.at[i]))
    sends = [
        pltpu.make_async_remote_copy(
            src_ref=mine,
            dst_ref=got.at[n],
            send_sem=send_sem.at[n],
            recv_sem=recv_sem.at[n],
            device_id=other,
            device_id_type=pl.DeviceIdType.MESH,
        )
        for n, other in enumerate(others)
    ]
    turns = [(cols - 1 - col) * send_last // (cols - 1) for col in range(cols)]
    for copy in (*loads[1:2], *loads[5:6], *reads[:1], *loads[:1], *loads[2:5], *loads[6:], *reads[1:ahead], *packs):
        copy.start()
    gains[...] = jnp.zeros_like(gains)
    loaded = set()
    for i, (n, at, piece) in enumerate(work):
        for col in range(cols):
            if turns[col] == i:

                @pl.when(leads & (my_col == col))
                def _():
                    pl.semaphore_wait(barrier, len(others))
                    for copy in sends:
                        copy.start()

        if n not in loaded:
            loaded.add(n)
            loads[n].wait()
            loads[4 + n].wait()
        reads[i].wait()
        if i + ahead < len(reads):
            reads[i + ahead].start()
        merge(*targets[n], held[n], lows[n], highs[n], at, piece)
    for copy in packs:
        copy.wait()

    @pl.when(leads)
    def _():
        for copy in sends:
            copy.wait()
        for zero in range(2):
            for n in range(cols):
                col = lax.rem(my_col + cols - n, cols)
                source = mine if n == 0 else got.at[n - 1]
                gains[pl.ds((zero * cols + col) * tall, tall), :] = source[pl.ds(zero * room, tall), :]

    for n in range(gains.shape[0] // gain_rows):
        part = gains[pl.ds(n * gain_rows, gain_rows), :].astype(jnp.bfloat16)
        mix_out[pl.ds(rows, gain_rows), pl.ds(n * lanes, lanes)] = part


def near_kernel(q_own, mix_own, m_own, far_m, low_m, high_m, q_out, k_out, v_out, m_out, done, own_sem, write_sem):
    slot = lax.axis_index("zero")
    rows, wide = k_out.shape[0] // 2, k_out.shape[1]
    writes = []
    for i, (source, target) in enumerate(
        (
            (m_own, place(m_out, slot, False, m_own.shape, 0, m_own.shape[0])),
            (q_own, place(q_out, slot, True, q_own.shape, 0, rows)),
            (mix_own.at[pl.ds(0, rows), pl.ds(0, wide)], place(k_out, slot, True, (rows, wide), 0, rows)),
            (mix_own.at[pl.ds(0, rows), pl.ds(wide, wide)], place(v_out, slot, True, (rows, wide), 0, rows)),
        )
    ):
        writes.append(pltpu.make_async_copy(source, target, own_sem.at[i]))
        writes[-1].start()
    merged = []
    for i, (at, tall) in enumerate(pieces_of(m_own.shape, write_bytes)):
        merge(done, 0, far_m, low_m, high_m, at, tall)
        target = place(m_out, 1 - slot, False, m_own.shape, at, tall)
        merged.append(pltpu.make_async_copy(done.at[pl.ds(at, tall), :], target, write_sem.at[i]))
        if i:
            merged[-2].start()
    merged[-1].start()
    for copy in (*writes, *merged):
        copy.wait()


def far_kernel(q_in, k_in, v_in, far_q, high_q, far_mix, mix_own, q_out, k_out, v_out, gain_out, gain, low_q, done, own_sem, write_sem):
    slot = lax.axis_index("zero")
    rows, wide = far_q.shape[0], k_out.shape[1]
    writes = []
    for i, out in enumerate((k_out, v_out)):
        source = far_mix.at[pl.ds(0, rows), pl.ds(i * wide, wide)]
        writes.append(pltpu.make_async_copy(source, place(out, 1 - slot, True, (rows, wide), 0, rows), own_sem.at[i]))
        writes[-1].start()
    for n in range(-(-gain.shape[0] // gain_rows)):
        where = (pl.ds(rows, gain_rows), pl.ds(n * lanes, lanes))
        tall = min(gain_rows, gain.shape[0] - n * gain_rows)
        part = jnp.where(slot == 1, mix_own[where], far_mix[where])
        gain[pl.ds(n * gain_rows, tall), :] = part[:tall]
    for i in range(rows // (2 * wide)):
        low_q[:, pl.ds(2 * i * wide, 2 * wide)] = far_mix[pl.ds(rows + gain_rows + i * rank, rank), :]
    merged = []
    for i, (at, tall) in enumerate(pieces_of(far_q.shape, write_bytes)):
        merge(done, 0, far_q, low_q, high_q, at, tall)
        target = place(q_out, 1 - slot, True, far_q.shape, at, tall)
        merged.append(pltpu.make_async_copy(done.at[pl.ds(at, tall), :], target, write_sem.at[i]))
        if i:
            merged[-2].start()
        else:
            writes.append(pltpu.make_async_copy(gain, gain_out, own_sem.at[2]))
            writes[-1].start()
    merged[-1].start()
    for copy in (*writes, *merged):
        copy.wait()


def cost_of(size, times):
    return pl.CostEstimate(flops=64 * size, bytes_accessed=times * size, transcendentals=0)


def paired(wq, lq, hq, wk, lk, hk, wv, lv, hv, wm, lm, hm, norm_train, norm_step):
    zeros, cols = lax.axis_size("zero"), lax.axis_size("cols")
    lq, lk, lv, lm = lq.T, lk.T, lv.T, lm.T
    total = (norm_train + norm_step).reshape(-1, lanes)

    def swap(x):
        return lax.ppermute(x, "zero", [(0, 1), (1, 0)])

    far_total = swap(total)
    far_wm, far_hm, far_wq = swap(wm), swap(hm), swap(wq)

    vmem, hbm = pl.BlockSpec(memory_space=pltpu.VMEM), pl.BlockSpec(memory_space=pl.ANY)
    far_off = lambda x: pltpu.with_memory_space_constraint(x, pltpu.HBM)
    near = lambda x: pltpu.with_memory_space_constraint(x, pltpu.VMEM)
    weights, factors = (wq, wk, wv, wm), (lq, lk, lv, lm, hq, hk, hv, hm)
    small = 6 * 2**20
    size = sum(w.size for w in weights)
    count = sum(len(pieces_of(w.shape, read_bytes)) for w in weights)
    tall = total.shape[0]
    room = -(-tall // 8) * 8
    whole_gain = zeros * cols * tall
    blocks = -(-whole_gain // gain_rows)
    wide = 2 * wk.shape[1]
    packs = wq.shape[0] // wide
    mix_shape = (wk.shape[0] + gain_rows + packs * rank, wide)
    bf16, f32 = jnp.bfloat16, jnp.float32
    own_q, own_mix, own_m, own_lm, own_hq = pl.pallas_call(
        functools.partial(own_kernel, cols),
        in_specs=[vmem] * 2 + [hbm] * 12,
        out_specs=[vmem] * 5,
        out_shape=[pltpu.VMEM(x, bf16) for x in (wq.shape, mix_shape, wm.shape, lm.shape, hq.shape)],
        scratch_shapes=[pltpu.VMEM(w.shape, bf16) for w in weights]
        + [pltpu.VMEM(x.shape, bf16) for x in (lq, lk, lv, hk, hv, hm)]
        + [pltpu.VMEM((2 * room, lanes), f32), pltpu.VMEM((cols - 1, 2 * room, lanes), f32)]
        + [pltpu.VMEM((blocks * gain_rows, lanes), f32)]
        + [pltpu.SemaphoreType.DMA((n,)) for n in (count, len(factors), packs, cols - 1, cols - 1)],
        compiler_params=pltpu.CompilerParams(
            vmem_limit_bytes=4 * size + small, collective_id=0, has_side_effects=True
        ),
        cost_estimate=cost_of(size, 2),
        name="own",
    )(*map(near, (total, far_total)), *map(far_off, (*weights, *factors)))
    far_mix = swap(near(own_mix))

    shapes = [jax.ShapeDtypeStruct((2 * w.shape[0], w.shape[1]), w.dtype) for w in weights[:3]]
    shapes.append(jax.ShapeDtypeStruct((wm.shape[0], 2 * wm.shape[1]), wm.dtype))
    out_q, out_k, out_v, out_m = pl.pallas_call(
        near_kernel,
        in_specs=[vmem] * 6,
        out_specs=[hbm] * 4,
        out_shape=shapes,
        scratch_shapes=[pltpu.VMEM(wm.shape, bf16), pltpu.SemaphoreType.DMA((4,))]
        + [pltpu.SemaphoreType.DMA((len(pieces_of(wm.shape, write_bytes)),))],
        compiler_params=pltpu.CompilerParams(vmem_limit_bytes=2 * wm.size + small),
        cost_estimate=cost_of(wm.size, 4),
        name="near",
    )(*map(near, (own_q, own_mix, own_m, far_wm, own_lm, far_hm)))
    out_q, out_k, out_v, gain = pl.pallas_call(
        far_kernel,
        in_specs=[hbm] * 3 + [vmem] * 4,
        out_specs=[hbm] * 4,
        out_shape=shapes[:3] + [jax.ShapeDtypeStruct((whole_gain, lanes), bf16)],
        input_output_aliases={0: 0, 1: 1, 2: 2},
        scratch_shapes=[pltpu.VMEM((whole_gain, lanes), bf16), pltpu.VMEM(lq.shape, bf16), pltpu.VMEM(wq.shape, bf16)]
        + [pltpu.SemaphoreType.DMA((3,))]
        + [pltpu.SemaphoreType.DMA((len(pieces_of(wq.shape, write_bytes)),))],
        compiler_params=pltpu.CompilerParams(vmem_limit_bytes=2 * wq.size + small),
        cost_estimate=cost_of(wq.size, 4),
        name="far",
    )(out_q, out_k, out_v, *map(near, (far_wq, own_hq, far_mix, own_mix)))
    return out_q, out_k, out_v, out_m, gain.reshape(-1)


def fits(mesh, args):
    if mesh.shape["zero"] != 2:
        return False
    wq, wk, wv, wm, gain = args[0], args[3], args[6], args[9], args[12]
    split = mesh.shape["zero"] * mesh.shape["job"]
    cols = mesh.shape["cols"]
    sizes = [w.shape[0] // split for w in (wq, wk, wv)] + [w.shape[1] // cols for w in (wq, wk, wv)]
    sizes += [wm.shape[0] // (mesh.shape["job"] * cols), wm.shape[1] // 2, gain.shape[0] // (split * cols)]
    return all(size % lanes == 0 for size in sizes)


def on_device(
    weight_query,
    low_query,
    high_query,
    weight_key,
    low_key,
    high_key,
    weight_value,
    low_value,
    high_value,
    weight_mixed,
    low_mixed,
    high_mixed,
    norm_train,
    norm_step,
):
    (
        moved_query,
        moved_key,
        moved_value,
        moved_mixed,
        factor_query,
        factor_key,
        factor_value,
        factor_mixed,
    ) = (
        lax.all_gather(weight_query, "zero", axis=0, tiled=True),
        lax.all_gather(weight_key, "zero", axis=0, tiled=True),
        lax.all_gather(weight_value, "zero", axis=0, tiled=True),
        lax.all_gather(weight_mixed, "zero", axis=1, tiled=True),
        lax.all_gather(low_query, "zero", axis=0, tiled=True),
        lax.all_gather(low_key, "zero", axis=0, tiled=True),
        lax.all_gather(low_value, "zero", axis=0, tiled=True),
        lax.all_gather(high_mixed, "zero", axis=1, tiled=True),
    )
    whole_query = moved_query.astype(jnp.float32) + mix_rate * jnp.dot(
        factor_query, high_query, preferred_element_type=jnp.float32
    )
    serving_query = whole_query.astype(jnp.bfloat16)
    whole_key = moved_key.astype(jnp.float32) + mix_rate * jnp.dot(
        factor_key, high_key, preferred_element_type=jnp.float32
    )
    serving_key = whole_key.astype(jnp.bfloat16)
    whole_value = moved_value.astype(jnp.float32) + mix_rate * jnp.dot(
        factor_value, high_value, preferred_element_type=jnp.float32
    )
    serving_value = whole_value.astype(jnp.bfloat16)
    whole_mixed = moved_mixed.astype(jnp.float32) + mix_rate * jnp.dot(
        low_mixed, factor_mixed, preferred_element_type=jnp.float32
    )
    serving_mixed = whole_mixed.astype(jnp.bfloat16)
    serve_norm = lax.all_gather(
        (norm_train + norm_step).astype(jnp.bfloat16), ("zero", "cols"), axis=0, tiled=True
    )
    return (serving_query, serving_key, serving_value, serving_mixed, serve_norm)


def solution(mesh):
    placed = (
        P(("job", "zero"), "cols"),
        P(("job", "zero"), None),
        P("job", "cols"),
        P(("job", "zero"), "cols"),
        P(("job", "zero"), None),
        P("job", "cols"),
        P(("job", "zero"), "cols"),
        P(("job", "zero"), None),
        P("job", "cols"),
        P(("job", "cols"), "zero"),
        P(("job", "cols"), None),
        P("job", "zero"),
        P(("job", "zero", "cols")),
        P(("job", "zero", "cols")),
    )
    sharded = functools.partial(
        jax.shard_map,
        mesh=mesh,
        in_specs=placed,
        out_specs=(
            P("job", "cols"),
            P("job", "cols"),
            P("job", "cols"),
            P(("job", "cols"), None),
            P("job"),
        ),
        check_vma=False,
    )

    def program(*args):
        if not fits(mesh, args):
            return sharded(on_device)(*args)

        return sharded(paired)(*args)

    return program
```

```python
import functools

import jax
import jax.numpy as jnp
from jax import lax
from jax.experimental import pallas as pl
from jax.experimental.pallas import tpu as pltpu
from jax.sharding import PartitionSpec as P


mix_rate = 2.0
lanes = 128
piece_bytes = 800 * 1024


tile_rows, tile_columns = 256, 256
own_order = (1, 2, 3, 0)
send_last, ahead, read_bytes = 2, 3, 2400 * 1024
write_bytes = 200 * 1024
gain_rows, rank = 16, 32


def merge(done, shift, weight, low_t, high, at, tall):
    columns = weight.shape[1]
    wide = tile_columns if columns % tile_columns == 0 else columns
    deep = tile_rows if tall % tile_rows == 0 else tall
    for top in range(at, at + tall, deep):
        low = low_t[:, pl.ds(top, deep)] * jnp.bfloat16(mix_rate)
        for left in range(0, columns, wide):
            where = (pl.ds(top, deep), pl.ds(left, wide))
            update = lax.dot_general(
                low, high[:, pl.ds(left, wide)], (((0,), (0,)), ((), ())), preferred_element_type=jnp.float32
            )
            done[pl.ds(top, deep), pl.ds(shift + left, wide)] = (weight[where].astype(jnp.float32) + update).astype(jnp.bfloat16)


def pieces_of(shape, limit=piece_bytes):
    rows, columns = shape
    best = lanes
    for tall in range(lanes, rows + 1, lanes):
        if rows % tall == 0 and 2 * tall * columns <= limit:
            best = tall
    return [(at, best) for at in range(0, rows, best)]


def place(whole, slot, by_rows, shape, at, tall):
    rows, columns = shape
    if by_rows:
        return whole.at[pl.ds(slot * rows + at, tall), :]
    return whole.at[pl.ds(at, tall), pl.ds(pl.multiple_of(slot * columns, lanes), columns)]


def own_kernel(cols, *refs):
    (total, far_total), weights, factors = refs[:2], refs[2:6], refs[6:14]
    q_out, mix_out, m_out, low_m, high_q = refs[14:19]
    held, lows, highs = refs[19:23], (*refs[23:26], low_m), (high_q, *refs[26:29])
    mine, got = refs[29:31]
    read_sem, factor_sem, pack_sem, send_sem, recv_sem = refs[31:]
    my_zero, my_col = lax.axis_index("zero"), lax.axis_index("cols")
    leads = my_zero == 1
    barrier = pltpu.get_barrier_semaphore()
    others = [{"cols": lax.rem(my_col + n, cols)} for n in range(1, cols)]

    @pl.when(leads)
    def _():
        for other in others:
            pl.semaphore_signal(barrier, inc=1, device_id=other, device_id_type=pl.DeviceIdType.MESH)

    tall = total.shape[0]
    room = mine.shape[0] // 2
    mine[pl.ds(my_zero * room, tall), :] = total[...]
    mine[pl.ds((1 - my_zero) * room, tall), :] = far_total[...]
    rows, wide = weights[1].shape
    targets = ((q_out, 0), (mix_out, 0), (mix_out, wide), (m_out, 0))
    work = [(n, at, tall) for n in own_order for at, tall in pieces_of(weights[n].shape, read_bytes)]
    reads = []
    for i, (n, at, piece) in enumerate(work):
        part = pl.ds(at, piece)
        reads.append(pltpu.make_async_copy(weights[n].at[part, :], held[n].at[part, :], read_sem.at[i]))
    loads = []
    for i, (source, target) in enumerate(zip(factors, (*lows, *highs))):
        loads.append(pltpu.make_async_copy(source, target, factor_sem.at[i]))
    below = rows + gain_rows
    packs = []
    for i in range(rows // (2 * wide)):
        target = mix_out.at[pl.ds(below + i * rank, rank), :]
        packs.append(pltpu.make_async_copy(factors[0].at[:, pl.ds(2 * i * wide, 2 * wide)], target, pack_sem.at[i]))
    sends = [
        pltpu.make_async_remote_copy(
            src_ref=mine,
            dst_ref=got.at[my_col],
            send_sem=send_sem.at[n],
            recv_sem=recv_sem.at[n],
            device_id=other,
            device_id_type=pl.DeviceIdType.MESH,
        )
        for n, other in enumerate(others)
    ]
    turns = [(cols - 1 - col) * send_last // (cols - 1) - (col == cols - 1) for col in range(cols)]
    starts_first = (lax.axis_index("job") == 0) & (my_col == 0)

    def send_when(here):
        @pl.when(leads & here)
        def _():
            pl.semaphore_wait(barrier, len(others))
            for copy in sends:
                copy.start()

    def send_on(turn):
        for col in range(cols):
            if turns[col] == turn:
                send_when((my_col == col) & jnp.logical_not(starts_first))

    send_on(-1)
    for copy in (*loads[1:2], *loads[5:6], *reads[:1], *loads[:1], *loads[2:5], *loads[6:], *reads[1:ahead], *packs):
        copy.start()
    mix_out[pl.ds(rows, gain_rows), :] = jnp.zeros((gain_rows, 2 * wide), jnp.bfloat16)
    loaded = set()
    for i, (n, at, piece) in enumerate(work):
        send_on(i)
        if n not in loaded:
            loaded.add(n)
            loads[n].wait()
            loads[4 + n].wait()
        reads[i].wait()
        if i + ahead < len(reads):
            reads[i + ahead].start()
        merge(*targets[n], held[n], lows[n], highs[n], at, piece)
    send_when(starts_first)
    for copy in packs:
        copy.wait()

    @pl.when(leads)
    def _():
        for copy in sends:
            copy.wait()
        for col in range(cols):
            mix_out[pl.ds(rows, gain_rows), pl.ds(col * lanes, lanes)] = got[col].astype(jnp.bfloat16)
        here = pl.ds(pl.multiple_of(my_col * lanes, lanes), lanes)
        mix_out[pl.ds(rows, gain_rows), here] = mine[...].astype(jnp.bfloat16)


def near_kernel(q_own, mix_own, m_own, far_m, low_m, high_m, q_out, k_out, v_out, m_out, done, own_sem, write_sem):
    slot = lax.axis_index("zero")
    rows, wide = k_out.shape[0] // 2, k_out.shape[1]
    writes = []
    for i, (source, target) in enumerate(
        (
            (m_own, place(m_out, slot, False, m_own.shape, 0, m_own.shape[0])),
            (q_own, place(q_out, slot, True, q_own.shape, 0, rows)),
            (mix_own.at[pl.ds(0, rows), pl.ds(0, wide)], place(k_out, slot, True, (rows, wide), 0, rows)),
            (mix_own.at[pl.ds(0, rows), pl.ds(wide, wide)], place(v_out, slot, True, (rows, wide), 0, rows)),
        )
    ):
        writes.append(pltpu.make_async_copy(source, target, own_sem.at[i]))
        writes[-1].start()
    merged = []
    for i, (at, tall) in enumerate(pieces_of(m_own.shape, write_bytes)):
        merge(done, 0, far_m, low_m, high_m, at, tall)
        target = place(m_out, 1 - slot, False, m_own.shape, at, tall)
        merged.append(pltpu.make_async_copy(done.at[pl.ds(at, tall), :], target, write_sem.at[i]))
        if i:
            merged[-2].start()
    merged[-1].start()
    for copy in (*writes, *merged):
        copy.wait()


def far_kernel(q_in, k_in, v_in, far_q, high_q, far_mix, mix_own, q_out, k_out, v_out, gain_out, gain, gain_half, low_q, done, own_sem, write_sem):
    slot = lax.axis_index("zero")
    rows, wide = far_q.shape[0], k_out.shape[1]
    writes = []
    for i, out in enumerate((k_out, v_out)):
        source = far_mix.at[pl.ds(0, rows), pl.ds(i * wide, wide)]
        writes.append(pltpu.make_async_copy(source, place(out, 1 - slot, True, (rows, wide), 0, rows), own_sem.at[i]))
        writes[-1].start()
    for i in range(rows // (2 * wide)):
        low_q[:, pl.ds(2 * i * wide, 2 * wide)] = far_mix[pl.ds(rows + gain_rows + i * rank, rank), :]
    merged = []
    for i, (at, tall) in enumerate(pieces_of(far_q.shape, write_bytes)):
        merge(done, 0, far_q, low_q, high_q, at, tall)
        target = place(q_out, 1 - slot, True, far_q.shape, at, tall)
        merged.append(pltpu.make_async_copy(done.at[pl.ds(at, tall), :], target, write_sem.at[i]))
        if i:
            merged[-2].start()
    merged[-1].start()
    where = (pl.ds(rows, gain_rows), slice(None))
    parts = jnp.where(slot == 1, mix_own[where], far_mix[where]).astype(jnp.float32)
    cols = 2 * wide // lanes
    tall, room = gain.shape[0] // (2 * cols), gain_rows // 2
    for zero in range(2):
        for col in range(cols):
            part = parts[zero * room : zero * room + tall, col * lanes : (col + 1) * lanes]
            gain[pl.ds((zero * cols + col) * tall, tall), :] = part
    gain_half[...] = gain[...].astype(jnp.bfloat16)
    writes.append(pltpu.make_async_copy(gain_half, gain_out, own_sem.at[2]))
    writes[-1].start()
    for copy in (*writes, *merged):
        copy.wait()


def cost_of(size, times):
    return pl.CostEstimate(flops=64 * size, bytes_accessed=times * size, transcendentals=0)


def paired(wq, lq, hq, wk, lk, hk, wv, lv, hv, wm, lm, hm, norm_train, norm_step):
    zeros, cols = lax.axis_size("zero"), lax.axis_size("cols")
    lq, lk, lv, lm = lq.T, lk.T, lv.T, lm.T
    total = (norm_train + norm_step).reshape(-1, lanes)

    def swap(x):
        return lax.ppermute(x, "zero", [(0, 1), (1, 0)])

    far_total = swap(total)
    far_wm, far_hm, far_wq = swap(wm), swap(hm), swap(wq)

    vmem, hbm = pl.BlockSpec(memory_space=pltpu.VMEM), pl.BlockSpec(memory_space=pl.ANY)
    far_off = lambda x: pltpu.with_memory_space_constraint(x, pltpu.HBM)
    near = lambda x: pltpu.with_memory_space_constraint(x, pltpu.VMEM)
    weights, factors = (wq, wk, wv, wm), (lq, lk, lv, lm, hq, hk, hv, hm)
    small = 6 * 2**20
    size = sum(w.size for w in weights)
    count = sum(len(pieces_of(w.shape, read_bytes)) for w in weights)
    tall = total.shape[0]
    room = gain_rows // 2
    whole_gain = zeros * cols * tall
    wide = 2 * wk.shape[1]
    packs = wq.shape[0] // wide
    mix_shape = (wk.shape[0] + gain_rows + packs * rank, wide)
    bf16, f32 = jnp.bfloat16, jnp.float32
    own_q, own_mix, own_m, own_lm, own_hq = pl.pallas_call(
        functools.partial(own_kernel, cols),
        in_specs=[vmem] * 2 + [hbm] * 12,
        out_specs=[vmem] * 5,
        out_shape=[pltpu.VMEM(x, bf16) for x in (wq.shape, mix_shape, wm.shape, lm.shape, hq.shape)],
        scratch_shapes=[pltpu.VMEM(w.shape, bf16) for w in weights]
        + [pltpu.VMEM(x.shape, bf16) for x in (lq, lk, lv, hk, hv, hm)]
        + [pltpu.VMEM((2 * room, lanes), f32), pltpu.VMEM((cols, 2 * room, lanes), f32)]
        + [pltpu.SemaphoreType.DMA((n,)) for n in (count, len(factors), packs, cols - 1, cols - 1)],
        compiler_params=pltpu.CompilerParams(
            vmem_limit_bytes=4 * size + small, collective_id=0, has_side_effects=True
        ),
        cost_estimate=cost_of(size, 2),
        name="own",
    )(*map(near, (total, far_total)), *map(far_off, (*weights, *factors)))
    far_mix = swap(near(own_mix))

    shapes = [jax.ShapeDtypeStruct((2 * w.shape[0], w.shape[1]), w.dtype) for w in weights[:3]]
    shapes.append(jax.ShapeDtypeStruct((wm.shape[0], 2 * wm.shape[1]), wm.dtype))
    out_q, out_k, out_v, out_m = pl.pallas_call(
        near_kernel,
        in_specs=[vmem] * 6,
        out_specs=[hbm] * 4,
        out_shape=shapes,
        scratch_shapes=[pltpu.VMEM(wm.shape, bf16), pltpu.SemaphoreType.DMA((4,))]
        + [pltpu.SemaphoreType.DMA((len(pieces_of(wm.shape, write_bytes)),))],
        compiler_params=pltpu.CompilerParams(vmem_limit_bytes=2 * wm.size + small),
        cost_estimate=cost_of(wm.size, 4),
        name="near",
    )(*map(near, (own_q, own_mix, own_m, far_wm, own_lm, far_hm)))
    out_q, out_k, out_v, gain = pl.pallas_call(
        far_kernel,
        in_specs=[hbm] * 3 + [vmem] * 4,
        out_specs=[hbm] * 4,
        out_shape=shapes[:3] + [jax.ShapeDtypeStruct((whole_gain, lanes), bf16)],
        input_output_aliases={0: 0, 1: 1, 2: 2},
        scratch_shapes=[pltpu.VMEM((whole_gain, lanes), f32), pltpu.VMEM((whole_gain, lanes), bf16)]
        + [pltpu.VMEM(lq.shape, bf16), pltpu.VMEM(wq.shape, bf16)]
        + [pltpu.SemaphoreType.DMA((3,))]
        + [pltpu.SemaphoreType.DMA((len(pieces_of(wq.shape, write_bytes)),))],
        compiler_params=pltpu.CompilerParams(vmem_limit_bytes=2 * wq.size + small),
        cost_estimate=cost_of(wq.size, 4),
        name="far",
    )(out_q, out_k, out_v, *map(near, (far_wq, own_hq, far_mix, own_mix)))
    return out_q, out_k, out_v, out_m, gain.reshape(-1)


def fits(mesh, args):
    if mesh.shape["zero"] != 2:
        return False
    wq, wk, wv, wm, gain = args[0], args[3], args[6], args[9], args[12]
    split = mesh.shape["zero"] * mesh.shape["job"]
    cols = mesh.shape["cols"]
    sizes = [w.shape[0] // split for w in (wq, wk, wv)] + [w.shape[1] // cols for w in (wq, wk, wv)]
    sizes += [wm.shape[0] // (mesh.shape["job"] * cols), wm.shape[1] // 2, gain.shape[0] // (split * cols)]
    tall = gain.shape[0] // (split * cols * lanes)
    return all(size % lanes == 0 for size in sizes) and 2 * sizes[4] == cols * lanes and tall <= gain_rows // 2


def on_device(
    weight_query,
    low_query,
    high_query,
    weight_key,
    low_key,
    high_key,
    weight_value,
    low_value,
    high_value,
    weight_mixed,
    low_mixed,
    high_mixed,
    norm_train,
    norm_step,
):
    (
        moved_query,
        moved_key,
        moved_value,
        moved_mixed,
        factor_query,
        factor_key,
        factor_value,
        factor_mixed,
    ) = (
        lax.all_gather(weight_query, "zero", axis=0, tiled=True),
        lax.all_gather(weight_key, "zero", axis=0, tiled=True),
        lax.all_gather(weight_value, "zero", axis=0, tiled=True),
        lax.all_gather(weight_mixed, "zero", axis=1, tiled=True),
        lax.all_gather(low_query, "zero", axis=0, tiled=True),
        lax.all_gather(low_key, "zero", axis=0, tiled=True),
        lax.all_gather(low_value, "zero", axis=0, tiled=True),
        lax.all_gather(high_mixed, "zero", axis=1, tiled=True),
    )
    whole_query = moved_query.astype(jnp.float32) + mix_rate * jnp.dot(
        factor_query, high_query, preferred_element_type=jnp.float32
    )
    serving_query = whole_query.astype(jnp.bfloat16)
    whole_key = moved_key.astype(jnp.float32) + mix_rate * jnp.dot(
        factor_key, high_key, preferred_element_type=jnp.float32
    )
    serving_key = whole_key.astype(jnp.bfloat16)
    whole_value = moved_value.astype(jnp.float32) + mix_rate * jnp.dot(
        factor_value, high_value, preferred_element_type=jnp.float32
    )
    serving_value = whole_value.astype(jnp.bfloat16)
    whole_mixed = moved_mixed.astype(jnp.float32) + mix_rate * jnp.dot(
        low_mixed, factor_mixed, preferred_element_type=jnp.float32
    )
    serving_mixed = whole_mixed.astype(jnp.bfloat16)
    serve_norm = lax.all_gather(
        (norm_train + norm_step).astype(jnp.bfloat16), ("zero", "cols"), axis=0, tiled=True
    )
    return (serving_query, serving_key, serving_value, serving_mixed, serve_norm)


def solution(mesh):
    placed = (
        P(("job", "zero"), "cols"),
        P(("job", "zero"), None),
        P("job", "cols"),
        P(("job", "zero"), "cols"),
        P(("job", "zero"), None),
        P("job", "cols"),
        P(("job", "zero"), "cols"),
        P(("job", "zero"), None),
        P("job", "cols"),
        P(("job", "cols"), "zero"),
        P(("job", "cols"), None),
        P("job", "zero"),
        P(("job", "zero", "cols")),
        P(("job", "zero", "cols")),
    )
    sharded = functools.partial(
        jax.shard_map,
        mesh=mesh,
        in_specs=placed,
        out_specs=(
            P("job", "cols"),
            P("job", "cols"),
            P("job", "cols"),
            P(("job", "cols"), None),
            P("job"),
        ),
        check_vma=False,
    )

    def program(*args):
        if not fits(mesh, args):
            return sharded(on_device)(*args)

        return sharded(paired)(*args)

    return program
```

```python
import functools

import jax
import jax.numpy as jnp
from jax import lax
from jax.experimental import pallas as pl
from jax.experimental.pallas import tpu as pltpu
from jax.sharding import PartitionSpec as P


mix_rate = 2.0
lanes = 128
piece_bytes = 800 * 1024


tile_rows, tile_columns = 256, 256
own_order = (1, 2, 3, 0)
ahead, read_bytes = 3, 2400 * 1024
write_bytes = 200 * 1024
gain_rows = 16


def merge(done, shift, weight, low_t, high, at, tall):
    columns = weight.shape[1]
    wide = tile_columns if columns % tile_columns == 0 else columns
    deep = tile_rows if tall % tile_rows == 0 else tall
    for top in range(at, at + tall, deep):
        low = low_t[:, pl.ds(top, deep)] * jnp.bfloat16(mix_rate)
        for left in range(0, columns, wide):
            where = (pl.ds(top, deep), pl.ds(left, wide))
            update = lax.dot_general(
                low, high[:, pl.ds(left, wide)], (((0,), (0,)), ((), ())), preferred_element_type=jnp.float32
            )
            done[pl.ds(top, deep), pl.ds(shift + left, wide)] = (weight[where].astype(jnp.float32) + update).astype(jnp.bfloat16)


def pieces_of(shape, limit=piece_bytes):
    rows, columns = shape
    best = lanes
    for tall in range(lanes, rows + 1, lanes):
        if rows % tall == 0 and 2 * tall * columns <= limit:
            best = tall
    return [(at, best) for at in range(0, rows, best)]


def place(whole, slot, by_rows, shape, at, tall):
    rows, columns = shape
    if by_rows:
        return whole.at[pl.ds(slot * rows + at, tall), :]
    return whole.at[pl.ds(at, tall), pl.ds(pl.multiple_of(slot * columns, lanes), columns)]


def own_kernel(cols, *refs):
    sources, weights, factors = refs[:2], refs[2:6], refs[6:14]
    q_out, mix_out, m_out, low_m, high_q = refs[14:19]
    held, lows, highs = refs[19:23], (*refs[23:26], low_m), (high_q, *refs[26:29])
    parts, mine, got = refs[29:32]
    read_sem, factor_sem, gain_sem, send_sem, recv_sem = refs[32:]
    my_zero, my_col = lax.axis_index("zero"), lax.axis_index("cols")
    leads = my_zero == 1
    barrier = pltpu.get_barrier_semaphore()
    others = [lax.rem(my_col + n, cols) for n in range(1, cols)]

    @pl.when(leads)
    def _():
        for col in others:
            for zero in range(2):
                where = {"zero": zero, "cols": col}
                pl.semaphore_signal(barrier, inc=1, device_id=where, device_id_type=pl.DeviceIdType.MESH)

    first_loads = [pltpu.make_async_copy(x, parts.at[i], gain_sem.at[i]) for i, x in enumerate(sources)]
    for copy in first_loads:
        copy.start()
    tall, room = parts.shape[1], mine.shape[0]
    rows, wide = weights[1].shape
    targets = ((q_out, 0), (mix_out, 0), (mix_out, wide), (m_out, 0))
    work = [(n, at, tall) for n in own_order for at, tall in pieces_of(weights[n].shape, read_bytes)]
    reads = []
    for i, (n, at, piece) in enumerate(work):
        part = pl.ds(at, piece)
        reads.append(pltpu.make_async_copy(weights[n].at[part, :], held[n].at[part, :], read_sem.at[i]))
    loads = []
    for i, (source, target) in enumerate(zip(factors, (*lows, *highs))):
        loads.append(pltpu.make_async_copy(source, target, factor_sem.at[i]))

    def moved(n, zero, source, target):
        there = pl.ds(pl.multiple_of(zero * room, room), room)
        return pltpu.make_async_remote_copy(
            src_ref=mine,
            dst_ref=got.at[source, there, :],
            send_sem=send_sem.at[n],
            recv_sem=recv_sem.at[zero * (cols - 1) + n],
            device_id={"zero": 1, "cols": target},
            device_id_type=pl.DeviceIdType.MESH,
        )

    sends = [moved(n, my_zero, my_col, col) for n, col in enumerate(others)]
    turns = [(cols - 1 - col) * 2 // (cols - 1) if 2 * col < cols else -1 for col in range(cols)]
    starts_first = (lax.axis_index("job") == 0) & (my_col == 0)

    def send_when(here):
        @pl.when(here)
        def _():
            pl.semaphore_wait(barrier, len(others))
            for copy in sends:
                copy.start()

    def send_on(turn):
        for col in range(cols):
            if turns[col] == turn:
                send_when((my_col == col) & jnp.logical_not(starts_first))

    for copy in first_loads:
        copy.wait()
    mine[...] = jnp.zeros_like(mine)
    mine[pl.ds(0, tall), :] = parts[0] + parts[1]
    send_on(-1)
    for copy in (*loads[1:2], *loads[5:6], *reads[:1], *loads[:1], *loads[2:5], *loads[6:], *reads[1:ahead]):
        copy.start()

    @pl.when(jnp.logical_not(leads))
    def _():
        got[...] = jnp.zeros_like(got)

    got[my_col] = jnp.zeros((2 * room, lanes), jnp.float32)
    got[my_col, pl.ds(pl.multiple_of(my_zero * room, room), room), :] = mine[...]
    loaded = set()
    for i, (n, at, piece) in enumerate(work):
        send_on(i)
        if n not in loaded:
            loaded.add(n)
            loads[n].wait()
            loads[4 + n].wait()
        reads[i].wait()
        if i + ahead < len(reads):
            reads[i + ahead].start()
        merge(*targets[n], held[n], lows[n], highs[n], at, piece)
    send_when(starts_first)
    for copy in sends:
        copy.wait_send()

    @pl.when(leads)
    def _():
        for zero in range(2):
            for n in range(cols - 1):
                moved(n, zero, lax.rem(my_col + cols - 1 - n, cols), my_col).wait_recv()

    for col in range(cols):
        mix_out[pl.ds(rows, gain_rows), pl.ds(col * lanes, lanes)] = got[col].astype(jnp.bfloat16)


def near_kernel(q_own, mix_own, m_own, far_m, low_m, high_m, q_out, k_out, v_out, m_out, done, own_sem, write_sem):
    slot = lax.axis_index("zero")
    rows, wide = k_out.shape[0] // 2, k_out.shape[1]
    writes = []
    for i, (source, target) in enumerate(
        (
            (m_own, place(m_out, slot, False, m_own.shape, 0, m_own.shape[0])),
            (q_own, place(q_out, slot, True, q_own.shape, 0, rows)),
            (mix_own.at[pl.ds(0, rows), pl.ds(0, wide)], place(k_out, slot, True, (rows, wide), 0, rows)),
            (mix_own.at[pl.ds(0, rows), pl.ds(wide, wide)], place(v_out, slot, True, (rows, wide), 0, rows)),
        )
    ):
        writes.append(pltpu.make_async_copy(source, target, own_sem.at[i]))
        writes[-1].start()
    merged = []
    for i, (at, tall) in enumerate(pieces_of(m_own.shape, write_bytes)):
        merge(done, 0, far_m, low_m, high_m, at, tall)
        target = place(m_out, 1 - slot, False, m_own.shape, at, tall)
        merged.append(pltpu.make_async_copy(done.at[pl.ds(at, tall), :], target, write_sem.at[i]))
        if i:
            merged[-2].start()
    merged[-1].start()
    for copy in (*writes, *merged):
        copy.wait()


def far_kernel(*refs):
    far_q, low_q, high_q, far_mix, mix_own, q_out, k_out, v_out, gain_out, gain, gain_half, done, own_sem, write_sem = refs[3:]
    slot = lax.axis_index("zero")
    rows, wide = far_q.shape[0], k_out.shape[1]
    writes = []
    for i, out in enumerate((k_out, v_out)):
        source = far_mix.at[pl.ds(0, rows), pl.ds(i * wide, wide)]
        writes.append(pltpu.make_async_copy(source, place(out, 1 - slot, True, (rows, wide), 0, rows), own_sem.at[i]))
        writes[-1].start()
    merged = []
    for i, (at, tall) in enumerate(pieces_of(far_q.shape, write_bytes)):
        merge(done, 0, far_q, low_q, high_q, at, tall)
        target = place(q_out, 1 - slot, True, far_q.shape, at, tall)
        merged.append(pltpu.make_async_copy(done.at[pl.ds(at, tall), :], target, write_sem.at[i]))
        if i:
            merged[-2].start()
    merged[-1].start()
    where = (pl.ds(rows, gain_rows), slice(None))
    parts = mix_own[where].astype(jnp.float32) + far_mix[where].astype(jnp.float32)
    cols = 2 * wide // lanes
    tall, room = gain.shape[0] // (2 * cols), gain_rows // 2
    for zero in range(2):
        for col in range(cols):
            part = parts[zero * room : zero * room + tall, col * lanes : (col + 1) * lanes]
            gain[pl.ds((zero * cols + col) * tall, tall), :] = part
    gain_half[...] = gain[...].astype(jnp.bfloat16)
    writes.append(pltpu.make_async_copy(gain_half, gain_out, own_sem.at[2]))
    writes[-1].start()
    for copy in (*writes, *merged):
        copy.wait()


def cost_of(size, times):
    return pl.CostEstimate(flops=64 * size, bytes_accessed=times * size, transcendentals=0)


def paired(wq, lq, hq, wk, lk, hk, wv, lv, hv, wm, lm, hm, norm_train, norm_step):
    zeros, cols = lax.axis_size("zero"), lax.axis_size("cols")
    lq, lk, lv, lm = lq.T, lk.T, lv.T, lm.T
    train, step = norm_train.reshape(-1, lanes), norm_step.reshape(-1, lanes)

    def swap(x):
        return lax.ppermute(x, "zero", [(0, 1), (1, 0)])

    far_wm, far_hm = swap(wm), swap(hm)
    far_wq, far_lq = swap(wq), swap(lq)

    vmem, hbm = pl.BlockSpec(memory_space=pltpu.VMEM), pl.BlockSpec(memory_space=pl.ANY)
    far_off = lambda x: pltpu.with_memory_space_constraint(x, pltpu.HBM)
    near = lambda x: pltpu.with_memory_space_constraint(x, pltpu.VMEM)
    weights, factors = (wq, wk, wv, wm), (lq, lk, lv, lm, hq, hk, hv, hm)
    small = 6 * 2**20
    size = sum(w.size for w in weights)
    count = sum(len(pieces_of(w.shape, read_bytes)) for w in weights)
    tall, room = train.shape[0], gain_rows // 2
    whole_gain = zeros * cols * tall
    wide = 2 * wk.shape[1]
    mix_shape = (wk.shape[0] + gain_rows, wide)
    bf16, f32 = jnp.bfloat16, jnp.float32
    own_q, own_mix, own_m, own_lm, own_hq = pl.pallas_call(
        functools.partial(own_kernel, cols),
        in_specs=[hbm] * 14,
        out_specs=[vmem] * 5,
        out_shape=[pltpu.VMEM(x, bf16) for x in (wq.shape, mix_shape, wm.shape, lm.shape, hq.shape)],
        scratch_shapes=[pltpu.VMEM(w.shape, bf16) for w in weights]
        + [pltpu.VMEM(x.shape, bf16) for x in (lq, lk, lv, hk, hv, hm)]
        + [pltpu.VMEM((2, tall, lanes), f32), pltpu.VMEM((room, lanes), f32), pltpu.VMEM((cols, 2 * room, lanes), f32)]
        + [pltpu.SemaphoreType.DMA((n,)) for n in (count, len(factors), 2, cols - 1, 2 * (cols - 1))],
        compiler_params=pltpu.CompilerParams(
            vmem_limit_bytes=4 * size + small, collective_id=0, has_side_effects=True
        ),
        cost_estimate=cost_of(size, 2),
        name="own",
    )(*map(far_off, (train, step, *weights, *factors)))
    far_mix = swap(near(own_mix))

    shapes = [jax.ShapeDtypeStruct((2 * w.shape[0], w.shape[1]), w.dtype) for w in weights[:3]]
    shapes.append(jax.ShapeDtypeStruct((wm.shape[0], 2 * wm.shape[1]), wm.dtype))
    out_q, out_k, out_v, out_m = pl.pallas_call(
        near_kernel,
        in_specs=[vmem] * 6,
        out_specs=[hbm] * 4,
        out_shape=shapes,
        scratch_shapes=[pltpu.VMEM(wm.shape, bf16), pltpu.SemaphoreType.DMA((4,))]
        + [pltpu.SemaphoreType.DMA((len(pieces_of(wm.shape, write_bytes)),))],
        compiler_params=pltpu.CompilerParams(vmem_limit_bytes=2 * wm.size + small),
        cost_estimate=cost_of(wm.size, 4),
        name="near",
    )(*map(near, (own_q, own_mix, own_m, far_wm, own_lm, far_hm)))
    out_q, out_k, out_v, gain = pl.pallas_call(
        far_kernel,
        in_specs=[hbm] * 3 + [vmem] * 5,
        out_specs=[hbm] * 4,
        out_shape=shapes[:3] + [jax.ShapeDtypeStruct((whole_gain, lanes), bf16)],
        input_output_aliases={0: 0, 1: 1, 2: 2},
        scratch_shapes=[pltpu.VMEM((whole_gain, lanes), f32), pltpu.VMEM((whole_gain, lanes), bf16)]
        + [pltpu.VMEM(wq.shape, bf16)]
        + [pltpu.SemaphoreType.DMA((3,))]
        + [pltpu.SemaphoreType.DMA((len(pieces_of(wq.shape, write_bytes)),))],
        compiler_params=pltpu.CompilerParams(vmem_limit_bytes=2 * wq.size + small),
        cost_estimate=cost_of(wq.size, 4),
        name="far",
    )(out_q, out_k, out_v, *map(near, (far_wq, far_lq, own_hq, far_mix, own_mix)))
    return out_q, out_k, out_v, out_m, gain.reshape(-1)


def fits(mesh, args):
    if mesh.shape["zero"] != 2:
        return False
    wq, wk, wv, wm, gain = args[0], args[3], args[6], args[9], args[12]
    split = mesh.shape["zero"] * mesh.shape["job"]
    cols = mesh.shape["cols"]
    sizes = [w.shape[0] // split for w in (wq, wk, wv)] + [w.shape[1] // cols for w in (wq, wk, wv)]
    sizes += [wm.shape[0] // (mesh.shape["job"] * cols), wm.shape[1] // 2, gain.shape[0] // (split * cols)]
    tall = gain.shape[0] // (split * cols * lanes)
    return all(size % lanes == 0 for size in sizes) and 2 * sizes[4] == cols * lanes and tall <= gain_rows // 2


def on_device(
    weight_query,
    low_query,
    high_query,
    weight_key,
    low_key,
    high_key,
    weight_value,
    low_value,
    high_value,
    weight_mixed,
    low_mixed,
    high_mixed,
    norm_train,
    norm_step,
):
    (
        moved_query,
        moved_key,
        moved_value,
        moved_mixed,
        factor_query,
        factor_key,
        factor_value,
        factor_mixed,
    ) = (
        lax.all_gather(weight_query, "zero", axis=0, tiled=True),
        lax.all_gather(weight_key, "zero", axis=0, tiled=True),
        lax.all_gather(weight_value, "zero", axis=0, tiled=True),
        lax.all_gather(weight_mixed, "zero", axis=1, tiled=True),
        lax.all_gather(low_query, "zero", axis=0, tiled=True),
        lax.all_gather(low_key, "zero", axis=0, tiled=True),
        lax.all_gather(low_value, "zero", axis=0, tiled=True),
        lax.all_gather(high_mixed, "zero", axis=1, tiled=True),
    )
    whole_query = moved_query.astype(jnp.float32) + mix_rate * jnp.dot(
        factor_query, high_query, preferred_element_type=jnp.float32
    )
    serving_query = whole_query.astype(jnp.bfloat16)
    whole_key = moved_key.astype(jnp.float32) + mix_rate * jnp.dot(
        factor_key, high_key, preferred_element_type=jnp.float32
    )
    serving_key = whole_key.astype(jnp.bfloat16)
    whole_value = moved_value.astype(jnp.float32) + mix_rate * jnp.dot(
        factor_value, high_value, preferred_element_type=jnp.float32
    )
    serving_value = whole_value.astype(jnp.bfloat16)
    whole_mixed = moved_mixed.astype(jnp.float32) + mix_rate * jnp.dot(
        low_mixed, factor_mixed, preferred_element_type=jnp.float32
    )
    serving_mixed = whole_mixed.astype(jnp.bfloat16)
    serve_norm = lax.all_gather(
        (norm_train + norm_step).astype(jnp.bfloat16), ("zero", "cols"), axis=0, tiled=True
    )
    return (serving_query, serving_key, serving_value, serving_mixed, serve_norm)


def solution(mesh):
    placed = (
        P(("job", "zero"), "cols"),
        P(("job", "zero"), None),
        P("job", "cols"),
        P(("job", "zero"), "cols"),
        P(("job", "zero"), None),
        P("job", "cols"),
        P(("job", "zero"), "cols"),
        P(("job", "zero"), None),
        P("job", "cols"),
        P(("job", "cols"), "zero"),
        P(("job", "cols"), None),
        P("job", "zero"),
        P(("job", "zero", "cols")),
        P(("job", "zero", "cols")),
    )
    sharded = functools.partial(
        jax.shard_map,
        mesh=mesh,
        in_specs=placed,
        out_specs=(
            P("job", "cols"),
            P("job", "cols"),
            P("job", "cols"),
            P(("job", "cols"), None),
            P("job"),
        ),
        check_vma=False,
    )

    def program(*args):
        if not fits(mesh, args):
            return sharded(on_device)(*args)

        return sharded(paired)(*args)

    return program
```

```python
import functools

import jax
import jax.numpy as jnp
from jax import lax
from jax.experimental import pallas as pl
from jax.experimental.pallas import tpu as pltpu
from jax.sharding import PartitionSpec as P


mix_rate = 2.0
lanes = 128
piece_bytes = 800 * 1024


tile_rows, tile_columns = 256, 256
own_order = (1, 2, 3, 0)
ahead, first_turn, relay_turn, read_bytes = 3, 3, 2, 2400 * 1024
write_bytes = 200 * 1024
gain_rows = 16


def merge(done, shift, weight, low_t, high, at, tall):
    columns = weight.shape[1]
    wide = tile_columns if columns % tile_columns == 0 else columns
    deep = tile_rows if tall % tile_rows == 0 else tall
    for top in range(at, at + tall, deep):
        low = low_t[:, pl.ds(top, deep)] * jnp.bfloat16(mix_rate)
        for left in range(0, columns, wide):
            where = (pl.ds(top, deep), pl.ds(left, wide))
            update = lax.dot_general(
                low, high[:, pl.ds(left, wide)], (((0,), (0,)), ((), ())), preferred_element_type=jnp.float32
            )
            done[pl.ds(top, deep), pl.ds(shift + left, wide)] = (weight[where].astype(jnp.float32) + update).astype(jnp.bfloat16)


def pieces_of(shape, limit=piece_bytes):
    rows, columns = shape
    best = lanes
    for tall in range(lanes, rows + 1, lanes):
        if rows % tall == 0 and 2 * tall * columns <= limit:
            best = tall
    return [(at, best) for at in range(0, rows, best)]


def place(whole, slot, by_rows, shape, at, tall):
    rows, columns = shape
    if by_rows:
        return whole.at[pl.ds(slot * rows + at, tall), :]
    return whole.at[pl.ds(at, tall), pl.ds(pl.multiple_of(slot * columns, lanes), columns)]


def own_kernel(cols, *refs):
    sources, weights, factors = refs[:2], refs[2:6], refs[6:14]
    q_out, mix_out, m_out, low_m, high_q = refs[14:19]
    held, lows, highs = refs[19:23], (*refs[23:26], low_m), (high_q, *refs[26:29])
    parts, mine, got = refs[29:32]
    read_sem, factor_sem, gain_sem, send_sem, recv_sem, relay_sem = refs[32:]
    last = cols - 1
    my_zero, my_col = lax.axis_index("zero"), lax.axis_index("cols")
    leads = my_zero == 1
    barrier = pltpu.get_barrier_semaphore()
    others = [lax.rem(my_col + n, cols) for n in range(1, cols)]

    first_loads = [pltpu.make_async_copy(x, parts.at[i], gain_sem.at[i]) for i, x in enumerate(sources)]
    for copy in first_loads:
        copy.start()

    @pl.when(leads)
    def _():
        for n, col in enumerate(others):

            @pl.when(jnp.logical_not((my_col == 1) & (n == 1) | (my_col == last) & (n == 0)))
            def _():
                for zero in range(2):
                    where = {"zero": zero, "cols": col}
                    pl.semaphore_signal(barrier, inc=1, device_id=where, device_id_type=pl.DeviceIdType.MESH)

    tall, room = parts.shape[1], mine.shape[0]
    rows, wide = weights[1].shape
    targets = ((q_out, 0), (mix_out, 0), (mix_out, wide), (m_out, 0))
    work = [(n, at, tall) for n in own_order for at, tall in pieces_of(weights[n].shape, read_bytes)]
    reads = []
    for i, (n, at, piece) in enumerate(work):
        part = pl.ds(at, piece)
        reads.append(pltpu.make_async_copy(weights[n].at[part, :], held[n].at[part, :], read_sem.at[i]))
    loads = []
    for i, (source, target) in enumerate(zip(factors, (*lows, *highs))):
        loads.append(pltpu.make_async_copy(source, target, factor_sem.at[i]))

    def moved(n, zero, source, target):
        there = pl.ds(pl.multiple_of(zero * room, room), room)
        return pltpu.make_async_remote_copy(
            src_ref=mine,
            dst_ref=got.at[source, there, :],
            send_sem=send_sem.at[n],
            recv_sem=recv_sem.at[zero * (cols - 1) + n],
            device_id={"zero": 1, "cols": target},
            device_id_type=pl.DeviceIdType.MESH,
        )

    sends = [moved(n, my_zero, my_col, col) for n, col in enumerate(others)]
    turns = [(cols - 1 - col) * 2 // (cols - 1) if 2 * col < cols else -1 for col in range(cols)]
    starts_first = (lax.axis_index("job") == 0) & (my_col == 0)

    def relay(source, target, i):
        return pltpu.make_async_remote_copy(
            src_ref=got.at[source],
            dst_ref=got.at[source],
            send_sem=relay_sem.at[2 * i],
            recv_sem=relay_sem.at[2 * i + 1],
            device_id={"zero": 1, "cols": target},
            device_id_type=pl.DeviceIdType.MESH,
        )

    back, onward = relay(last, 1, 0), relay(0, last, 1)
    skips = {0: (last - 1,), last: (1,)}

    def send_when(here, skip=()):
        @pl.when(here)
        def _():
            pl.semaphore_wait(barrier, len(others) - len(skip))
            for n, copy in enumerate(sends):
                if n not in skip:
                    copy.start()

    def send_on(turn):
        for col in range(cols):
            if turns[col] == turn:
                send_when((my_col == col) & jnp.logical_not(starts_first), skips.get(col, ()))

    def arrived(n):
        for zero in range(2):
            moved(n, zero, lax.rem(my_col + cols - 1 - n, cols), my_col).wait_recv()

    def pass_on():
        @pl.when(leads & (my_col == last - 1))
        def _():
            arrived(last - 1)
            back.start()

    late = 2 * my_col >= cols

    def read_ahead():
        for copy in (*loads[1:2], *loads[5:6], *reads[:1], *loads[:1], *loads[2:5], *loads[6:], *reads[1:ahead]):
            copy.start()

    @pl.when(jnp.logical_not(late))
    def _():
        read_ahead()

    for copy in first_loads:
        copy.wait()
    mine[...] = jnp.zeros_like(mine)
    mine[pl.ds(0, tall), :] = parts[0] + parts[1]
    send_on(-1)

    @pl.when(late)
    def _():
        read_ahead()

    @pl.when(jnp.logical_not(leads))
    def _():
        got[...] = jnp.zeros_like(got)

    got[my_col] = jnp.zeros((2 * room, lanes), jnp.float32)
    got[my_col, pl.ds(pl.multiple_of(my_zero * room, room), room), :] = mine[...]
    loaded = set()
    for i, (n, at, piece) in enumerate(work):
        send_on(i)
        if i == first_turn:
            send_when(starts_first, skips[0])
        if i == relay_turn:
            pass_on()
        if i == first_turn:

            @pl.when(leads & (my_col == last - 1))
            def _():
                arrived(1)
                onward.start()

        if n not in loaded:
            loaded.add(n)
            loads[n].wait()
            loads[4 + n].wait()
        reads[i].wait()
        if i + ahead < len(reads):
            reads[i + ahead].start()
        merge(*targets[n], held[n], lows[n], highs[n], at, piece)

    for n, copy in enumerate(sends):

        @pl.when(jnp.logical_not((my_col == last) & (n == 1) | (my_col == 0) & (n == last - 1)))
        def _():
            copy.wait_send()

    for n in range(cols - 1):

        direct = jnp.logical_not((my_col == 1) & (n == 1) | (my_col == last) & (n == last - 1) | (my_col == last - 1) & (n > 0))

        @pl.when(leads & direct)
        def _():
            arrived(n)

    @pl.when(leads & (my_col == 1))
    def _():
        back.wait_recv()

    @pl.when(leads & (my_col == last))
    def _():
        onward.wait_recv()

    @pl.when(leads & (my_col == last - 1))
    def _():
        back.wait_send()
        onward.wait_send()

    for col in range(cols):
        mix_out[pl.ds(rows, gain_rows), pl.ds(col * lanes, lanes)] = got[col].astype(jnp.bfloat16)


def waits_long():
    return (lax.axis_index("job") == 0) & (lax.axis_index("cols") == 0) & (lax.axis_index("zero") == 0)


def own_query(q_own, q_out, sem):
    place_own = place(q_out, lax.axis_index("zero"), True, q_own.shape, 0, q_own.shape[0])
    return pltpu.make_async_copy(q_own, place_own, sem)


def early_kernel(q_own, q_out, sem):
    @pl.when(waits_long())
    def _():
        copy = own_query(q_own, q_out, sem)
        copy.start()
        copy.wait()


def near_kernel(q_in, q_own, mix_own, m_own, far_m, low_m, high_m, q_out, k_out, v_out, m_out, done, own_sem, write_sem):
    slot = lax.axis_index("zero")
    rows, wide = k_out.shape[0] // 2, k_out.shape[1]
    writes = []
    for i, (source, target) in enumerate(
        (
            (m_own, place(m_out, slot, False, m_own.shape, 0, m_own.shape[0])),
            (mix_own.at[pl.ds(0, rows), pl.ds(0, wide)], place(k_out, slot, True, (rows, wide), 0, rows)),
            (mix_own.at[pl.ds(0, rows), pl.ds(wide, wide)], place(v_out, slot, True, (rows, wide), 0, rows)),
        )
    ):
        writes.append(pltpu.make_async_copy(source, target, own_sem.at[i]))
        writes[-1].start()
    query = own_query(q_own, q_out, own_sem.at[3])

    @pl.when(jnp.logical_not(waits_long()))
    def _():
        query.start()

    merged = []
    for i, (at, tall) in enumerate(pieces_of(m_own.shape, write_bytes)):
        merge(done, 0, far_m, low_m, high_m, at, tall)
        target = place(m_out, 1 - slot, False, m_own.shape, at, tall)
        merged.append(pltpu.make_async_copy(done.at[pl.ds(at, tall), :], target, write_sem.at[i]))
        if i:
            merged[-2].start()
    merged[-1].start()
    for copy in (*writes, *merged):
        copy.wait()

    @pl.when(jnp.logical_not(waits_long()))
    def _():
        query.wait()


def far_kernel(*refs):
    far_q, low_q, high_q, far_mix, mix_own, q_out, k_out, v_out, gain_out, gain, gain_half, done, own_sem, write_sem = refs[3:]
    slot = lax.axis_index("zero")
    rows, wide = far_q.shape[0], k_out.shape[1]
    writes = []
    for i, out in enumerate((k_out, v_out)):
        source = far_mix.at[pl.ds(0, rows), pl.ds(i * wide, wide)]
        writes.append(pltpu.make_async_copy(source, place(out, 1 - slot, True, (rows, wide), 0, rows), own_sem.at[i]))
        writes[-1].start()
    merged = []
    for i, (at, tall) in enumerate(pieces_of(far_q.shape, write_bytes)):
        merge(done, 0, far_q, low_q, high_q, at, tall)
        target = place(q_out, 1 - slot, True, far_q.shape, at, tall)
        merged.append(pltpu.make_async_copy(done.at[pl.ds(at, tall), :], target, write_sem.at[i]))
        if i:
            merged[-2].start()
    merged[-1].start()
    where = (pl.ds(rows, gain_rows), slice(None))
    parts = mix_own[where].astype(jnp.float32) + far_mix[where].astype(jnp.float32)
    cols = 2 * wide // lanes
    tall, room = gain.shape[0] // (2 * cols), gain_rows // 2
    for zero in range(2):
        for col in range(cols):
            part = parts[zero * room : zero * room + tall, col * lanes : (col + 1) * lanes]
            gain[pl.ds((zero * cols + col) * tall, tall), :] = part
    gain_half[...] = gain[...].astype(jnp.bfloat16)
    writes.append(pltpu.make_async_copy(gain_half, gain_out, own_sem.at[2]))
    writes[-1].start()
    for copy in (*writes, *merged):
        copy.wait()


def cost_of(size, times):
    return pl.CostEstimate(flops=64 * size, bytes_accessed=times * size, transcendentals=0)


def paired(wq, lq, hq, wk, lk, hk, wv, lv, hv, wm, lm, hm, norm_train, norm_step):
    zeros, cols = lax.axis_size("zero"), lax.axis_size("cols")
    lq, lk, lv, lm = lq.T, lk.T, lv.T, lm.T
    train, step = norm_train.reshape(-1, lanes), norm_step.reshape(-1, lanes)

    def swap(x):
        return lax.ppermute(x, "zero", [(0, 1), (1, 0)])

    far_wm, far_hm = swap(wm), swap(hm)
    far_wq, far_lq = swap(wq), swap(lq)

    vmem, hbm = pl.BlockSpec(memory_space=pltpu.VMEM), pl.BlockSpec(memory_space=pl.ANY)
    far_off = lambda x: pltpu.with_memory_space_constraint(x, pltpu.HBM)
    near = lambda x: pltpu.with_memory_space_constraint(x, pltpu.VMEM)
    weights, factors = (wq, wk, wv, wm), (lq, lk, lv, lm, hq, hk, hv, hm)
    small = 6 * 2**20
    size = sum(w.size for w in weights)
    count = sum(len(pieces_of(w.shape, read_bytes)) for w in weights)
    tall, room = train.shape[0], gain_rows // 2
    whole_gain = zeros * cols * tall
    wide = 2 * wk.shape[1]
    mix_shape = (wk.shape[0] + gain_rows, wide)
    bf16, f32 = jnp.bfloat16, jnp.float32
    own_q, own_mix, own_m, own_lm, own_hq = pl.pallas_call(
        functools.partial(own_kernel, cols),
        in_specs=[hbm] * 14,
        out_specs=[vmem] * 5,
        out_shape=[pltpu.VMEM(x, bf16) for x in (wq.shape, mix_shape, wm.shape, lm.shape, hq.shape)],
        scratch_shapes=[pltpu.VMEM(w.shape, bf16) for w in weights]
        + [pltpu.VMEM(x.shape, bf16) for x in (lq, lk, lv, hk, hv, hm)]
        + [pltpu.VMEM((2, tall, lanes), f32), pltpu.VMEM((room, lanes), f32), pltpu.VMEM((cols, 2 * room, lanes), f32)]
        + [pltpu.SemaphoreType.DMA((n,)) for n in (count, len(factors), 2, cols - 1, 2 * (cols - 1), 4)],
        compiler_params=pltpu.CompilerParams(
            vmem_limit_bytes=4 * size + small, collective_id=0, has_side_effects=True
        ),
        cost_estimate=cost_of(size, 2),
        name="own",
    )(*map(far_off, (train, step, *weights, *factors)))

    shapes = [jax.ShapeDtypeStruct((2 * w.shape[0], w.shape[1]), w.dtype) for w in weights[:3]]
    shapes.append(jax.ShapeDtypeStruct((wm.shape[0], 2 * wm.shape[1]), wm.dtype))
    out_q = pl.pallas_call(
        early_kernel,
        in_specs=[vmem],
        out_specs=hbm,
        out_shape=shapes[0],
        scratch_shapes=[pltpu.SemaphoreType.DMA],
        compiler_params=pltpu.CompilerParams(vmem_limit_bytes=small),
        cost_estimate=cost_of(wm.size, 1),
        name="early",
    )(near(own_q))
    far_mix = swap(near(own_mix))
    out_q, out_k, out_v, out_m = pl.pallas_call(
        near_kernel,
        in_specs=[hbm] + [vmem] * 6,
        out_specs=[hbm] * 4,
        out_shape=shapes,
        scratch_shapes=[pltpu.VMEM(wm.shape, bf16), pltpu.SemaphoreType.DMA((4,))]
        + [pltpu.SemaphoreType.DMA((len(pieces_of(wm.shape, write_bytes)),))],
        compiler_params=pltpu.CompilerParams(vmem_limit_bytes=2 * wm.size + small),
        cost_estimate=cost_of(wm.size, 4),
        input_output_aliases={0: 0},
        name="near",
    )(out_q, *map(near, (own_q, own_mix, own_m, far_wm, own_lm, far_hm)))
    out_q, out_k, out_v, gain = pl.pallas_call(
        far_kernel,
        in_specs=[hbm] * 3 + [vmem] * 5,
        out_specs=[hbm] * 4,
        out_shape=shapes[:3] + [jax.ShapeDtypeStruct((whole_gain, lanes), bf16)],
        input_output_aliases={0: 0, 1: 1, 2: 2},
        scratch_shapes=[pltpu.VMEM((whole_gain, lanes), f32), pltpu.VMEM((whole_gain, lanes), bf16)]
        + [pltpu.VMEM(wq.shape, bf16)]
        + [pltpu.SemaphoreType.DMA((3,))]
        + [pltpu.SemaphoreType.DMA((len(pieces_of(wq.shape, write_bytes)),))],
        compiler_params=pltpu.CompilerParams(vmem_limit_bytes=2 * wq.size + small),
        cost_estimate=cost_of(wq.size, 4),
        name="far",
    )(out_q, out_k, out_v, *map(near, (far_wq, far_lq, own_hq, far_mix, own_mix)))
    return out_q, out_k, out_v, out_m, gain.reshape(-1)


def fits(mesh, args):
    if mesh.shape["zero"] != 2 or mesh.shape["cols"] != 4:
        return False
    wq, wk, wv, wm, gain = args[0], args[3], args[6], args[9], args[12]
    split = mesh.shape["zero"] * mesh.shape["job"]
    cols = mesh.shape["cols"]
    sizes = [w.shape[0] // split for w in (wq, wk, wv)] + [w.shape[1] // cols for w in (wq, wk, wv)]
    sizes += [wm.shape[0] // (mesh.shape["job"] * cols), wm.shape[1] // 2, gain.shape[0] // (split * cols)]
    tall = gain.shape[0] // (split * cols * lanes)
    return all(size % lanes == 0 for size in sizes) and 2 * sizes[4] == cols * lanes and tall <= gain_rows // 2


def on_device(
    weight_query,
    low_query,
    high_query,
    weight_key,
    low_key,
    high_key,
    weight_value,
    low_value,
    high_value,
    weight_mixed,
    low_mixed,
    high_mixed,
    norm_train,
    norm_step,
):
    (
        moved_query,
        moved_key,
        moved_value,
        moved_mixed,
        factor_query,
        factor_key,
        factor_value,
        factor_mixed,
    ) = (
        lax.all_gather(weight_query, "zero", axis=0, tiled=True),
        lax.all_gather(weight_key, "zero", axis=0, tiled=True),
        lax.all_gather(weight_value, "zero", axis=0, tiled=True),
        lax.all_gather(weight_mixed, "zero", axis=1, tiled=True),
        lax.all_gather(low_query, "zero", axis=0, tiled=True),
        lax.all_gather(low_key, "zero", axis=0, tiled=True),
        lax.all_gather(low_value, "zero", axis=0, tiled=True),
        lax.all_gather(high_mixed, "zero", axis=1, tiled=True),
    )
    whole_query = moved_query.astype(jnp.float32) + mix_rate * jnp.dot(
        factor_query, high_query, preferred_element_type=jnp.float32
    )
    serving_query = whole_query.astype(jnp.bfloat16)
    whole_key = moved_key.astype(jnp.float32) + mix_rate * jnp.dot(
        factor_key, high_key, preferred_element_type=jnp.float32
    )
    serving_key = whole_key.astype(jnp.bfloat16)
    whole_value = moved_value.astype(jnp.float32) + mix_rate * jnp.dot(
        factor_value, high_value, preferred_element_type=jnp.float32
    )
    serving_value = whole_value.astype(jnp.bfloat16)
    whole_mixed = moved_mixed.astype(jnp.float32) + mix_rate * jnp.dot(
        low_mixed, factor_mixed, preferred_element_type=jnp.float32
    )
    serving_mixed = whole_mixed.astype(jnp.bfloat16)
    serve_norm = lax.all_gather(
        (norm_train + norm_step).astype(jnp.bfloat16), ("zero", "cols"), axis=0, tiled=True
    )
    return (serving_query, serving_key, serving_value, serving_mixed, serve_norm)


def solution(mesh):
    placed = (
        P(("job", "zero"), "cols"),
        P(("job", "zero"), None),
        P("job", "cols"),
        P(("job", "zero"), "cols"),
        P(("job", "zero"), None),
        P("job", "cols"),
        P(("job", "zero"), "cols"),
        P(("job", "zero"), None),
        P("job", "cols"),
        P(("job", "cols"), "zero"),
        P(("job", "cols"), None),
        P("job", "zero"),
        P(("job", "zero", "cols")),
        P(("job", "zero", "cols")),
    )
    sharded = functools.partial(
        jax.shard_map,
        mesh=mesh,
        in_specs=placed,
        out_specs=(
            P("job", "cols"),
            P("job", "cols"),
            P("job", "cols"),
            P(("job", "cols"), None),
            P("job"),
        ),
        check_vma=False,
    )

    def program(*args):
        if not fits(mesh, args):
            return sharded(on_device)(*args)

        return sharded(paired)(*args)

    return program
```
